32 devices in a mesh: dp: 4 (over y, x), mp: 8 (over z, core).
Axes of the slice: x: 2, y: 2, z: 4, core: 2. Of those that a mesh axis runs over, the one named last changes fastest.
Arguments:
- stored: float32 [16384, 18432], P(('dp', 'mp')), may hold values from -0.046875 to 0.046875
- row_map: int32 [16384], replicated, may hold values from 0 to 16383, as said below
- probe: bfloat16 [16384, 1024], P('dp'), may hold values from -6 to 6
- lane: bfloat16 [128, 1024], replicated, may hold values from -6 to 6
Outputs:
- shards: bfloat16 [144, 128, 16384], P('mp', None, 'dp')
- slab_checks: float32 [144, 32, 1024], P('mp', 'dp')
- head_sums: float32 [144, 1024], P('mp')
The draws below stay inside these ranges and needn't reach their ends.
Inputs may be any that keep to these rules, and one draw needn't show every extreme that they name: row_map is a permutation of 0..16383 with row_map[i] // 4096 == (i % 512) // 128 for every stored row i.
All inputs are finite; a program needn't handle non-finite values.
Results may differ from the reference program's by a relative error of at most 0.0029.
Values may be sent and summed in bfloat16 or wider, within the bound.
A program may use at most 128 MiB of HBM per device.

```python
import jax
import jax.numpy as jnp
from jax import lax

D = 16384
Q_HEADS = 128
KV_HEADS = 8
HD = 128
PROBES = 1024
SLABS = 8
QKV = 18432
ROWS_DEV = 512
SUB_ROWS = 128
GROUP_ROWS = 4096
DP_GROUPS = 4
SLAB = 512
SLOTS = 18
N_DP = 4
N_MP = 8


def draw_row_map(key, part):
    stored_index = jnp.arange(D, dtype=jnp.int32)
    target_group = stored_index % ROWS_DEV // SUB_ROWS
    rank_inside = stored_index // ROWS_DEV * SUB_ROWS + stored_index % SUB_ROWS
    group_keys = jax.random.split(jax.random.fold_in(key, 17), DP_GROUPS)
    shuffled = jax.vmap(lambda one_key: jax.random.permutation(one_key, GROUP_ROWS))(group_keys).astype(jnp.int32)
    return (target_group * GROUP_ROWS + shuffled[target_group, rank_inside]).astype(jnp.int32)


def levels(rng, dims, pieces, least, high):
    def one(axis_at, blocks):
        heights = jax.random.uniform(jax.random.fold_in(jax.random.fold_in(rng, 6), axis_at), (blocks,), jnp.float32, least / len(pieces), high / len(pieces))
        return jnp.repeat(jnp.exp(heights), dims[axis_at] // blocks).reshape((-1,) + (1,) * (len(dims) - axis_at - 1))

    factor_of = one(*pieces[0])
    for cut in pieces[1:]:
        factor_of = factor_of * one(*cut)
    return factor_of


def scatter_about(stream_key, dims, deviation, reach, cuts=(), kind=jnp.bfloat16):
    entries = deviation * jax.random.normal(stream_key, dims, jnp.float32)
    if cuts:
        entries = entries * levels(stream_key, dims, cuts, -0.22, 0.18)
    return jnp.clip(entries, -reach, reach).astype(kind)


def setup_inputs(seed: int = 0) -> dict:
    arg_keys = jax.random.split(jax.random.key(seed), 5)
    return {
        "stored": scatter_about(arg_keys[0], (D, QKV), D ** -0.5, 0.046875, ((0, 32),), jnp.float32),
        "row_map": draw_row_map(jax.random.fold_in(arg_keys[4], 71), 0),
        "probe": scatter_about(arg_keys[2], (D, PROBES), 1.0, 6.0, ((0, 4),)),
        "lane": scatter_about(arg_keys[3], (HD, PROBES), 1.0, 6.0),
    }


def reference(stored, row_map, probe, lane):
    weights = jnp.zeros((D, QKV), jnp.bfloat16).at[row_map].set(stored.astype(jnp.bfloat16))
    head_cols = weights.reshape(D, Q_HEADS + 2 * KV_HEADS, HD)
    kv_index = (jnp.arange(N_MP, dtype=jnp.int32) * KV_HEADS) // N_MP
    query_cols = head_cols[:, :Q_HEADS].reshape(D, N_MP, Q_HEADS // N_MP, HD)
    key_cols = head_cols[:, Q_HEADS + kv_index][:, :, None]
    value_cols = head_cols[:, Q_HEADS + KV_HEADS + kv_index][:, :, None]
    slotted = jnp.concatenate([query_cols, key_cols, value_cols], axis=2)
    shards = jnp.transpose(slotted, (1, 2, 3, 0)).reshape(N_MP * SLOTS, HD, D)
    lane_wide = lane.astype(jnp.float32)

    def one_slab(slab_start):
        slab_block = lax.dynamic_slice_in_dim(shards, slab_start, SLAB, 2).astype(jnp.float32)
        probe_rows = lax.dynamic_slice_in_dim(probe, slab_start, SLAB, 0).astype(jnp.float32)
        projected = jnp.einsum("jer,rp->jep", slab_block, probe_rows, precision=lax.Precision.HIGHEST)
        return jnp.sum(projected * lane_wide[None], axis=1)

    slab_starts = jnp.arange(N_DP * SLABS, dtype=jnp.int32) * SLAB
    stacked = lax.map(one_slab, slab_starts)
    slab_checks = jnp.transpose(stacked, (1, 0, 2))
    head_sums = jnp.mean(slab_checks, axis=1)
    return shards, slab_checks, head_sums
```

```python
import functools

import jax
import jax.numpy as jnp
from jax import lax
from jax.experimental import pallas as pl
from jax.experimental.pallas import tpu as pltpu
from jax.sharding import PartitionSpec as P

Q_HEADS = 128
KV_HEADS = 8
HD = 128
SLABS = 8
PAIR = 2
AHEAD = 3
UNROLL = 4
MESH = pl.DeviceIdType.MESH


def exchange(
    n_dp, n_mp, stored, row_map, probe_any, lane_any,
    shards, checks, heads, landing,
    narrow, wide, bufs, turned, acc, probe, lane, table, offset, slab_sums, sums, tail_sums,
    load_sem, aux_sem, fetch_sem, send_sem, recv_sem, sum_send, sum_recv, tail_send, tail_recv,
):
    my_dp = lax.axis_index("dp")
    my_mp = lax.axis_index("mp")
    n_dev = n_dp * n_mp
    rows_dev = stored.shape[0]
    sub = rows_dev // n_dp
    group_rows = probe.shape[0]
    slab_rows = group_rows // SLABS
    per_device = Q_HEADS // n_mp
    slots = per_device + 2
    share = n_mp // KV_HEADS
    chunks = slots // PAIR
    last = chunks - 1
    width = PAIR * HD
    half = n_mp // 2
    my_half = my_mp // half
    part_rows = n_dp * sub
    ahead = min(AHEAD, chunks)
    last_slot = (last * PAIR + per_device) % slots

    def peer_mp(i):
        other = i // half
        side = (1 - my_half) * (1 - other) + my_half * other
        return side * half + lax.rem(my_mp + i, half)

    def group_mp(i):
        far = i // half
        inner = lax.rem(i, half)
        own = my_half * half + lax.rem(my_mp + inner, half)
        other = my_half * inner + (1 - my_half) * (n_mp - 1 - inner)
        return own * (1 - far) + other * far

    def load(step, i):
        mp = peer_mp(i)
        if isinstance(step, int) and step == 0:
            for pos, head in enumerate((Q_HEADS + mp // share, Q_HEADS + KV_HEADS + mp // share)):
                first = pl.multiple_of(head * HD, HD)
                src = stored.at[:, pl.ds(first, HD)]
                pltpu.make_async_copy(src, wide.at[i, :, pl.ds(pos * HD, HD)], load_sem.at[i]).start()
        else:
            first = pl.multiple_of((mp * per_device + (step - 1) * PAIR) * HD, HD)
            pltpu.make_async_copy(stored.at[:, pl.ds(first, width)], wide.at[i], load_sem.at[i]).start()

    def issue(step):
        @pl.loop(0, n_mp)
        def _(i):
            mp = peer_mp(i)
            pltpu.make_async_copy(wide.at[i], wide.at[i], load_sem.at[i]).wait()

            @pl.loop(0, n_dp)
            def _(d):
                narrow[step, mp, d] = wide[i, pl.ds(pl.multiple_of(d * sub, sub), sub), :].astype(jnp.bfloat16)

            @pl.loop(0, n_dp)
            def _(a):
                @pl.when(i * n_dp + a != half * n_dp)
                def _():
                    dp = lax.rem(my_dp + a, n_dp)

                    def send(target):
                        pltpu.make_async_remote_copy(
                            src_ref=narrow.at[step, mp, dp],
                            dst_ref=target,
                            send_sem=send_sem.at[step],
                            recv_sem=recv_sem.at[step, my_mp],
                            device_id=(dp, mp),
                            device_id_type=MESH,
                        ).start()

                    if isinstance(step, int):
                        send(bufs.at[1, my_mp, my_dp] if step == last else landing.at[step, my_mp, my_dp])
                    else:
                        @pl.when(step < last)
                        def _():
                            send(landing.at[step, my_mp, my_dp])

                        @pl.when(step == last)
                        def _():
                            send(bufs.at[1, my_mp, my_dp])

            if isinstance(step, int):
                if step < last:
                    load(step + 1, i)
            else:
                @pl.when(step < last)
                def _():
                    load(step + 1, i)

    @pl.loop(0, n_mp)
    def _(i):
        load(0, i)

    barrier = pltpu.get_barrier_semaphore()

    @pl.loop(1, n_dev)
    def _(k):
        other = (lax.rem(my_dp + k // n_mp, n_dp), lax.rem(my_mp + lax.rem(k, n_mp), n_mp))
        pl.semaphore_signal(barrier, inc=1, device_id=other, device_id_type=MESH)

    aux = (
        pltpu.make_async_copy(row_map, table, aux_sem.at[0]),
        pltpu.make_async_copy(lane_any, lane, aux_sem.at[1]),
        pltpu.make_async_copy(probe_any, probe, aux_sem.at[2]),
    )
    pl.semaphore_wait(barrier, n_dev - 1)
    issue(0)
    for copy in aux:
        copy.start()
    for step in range(1, ahead):
        issue(step)

    for copy in aux:
        copy.wait()
    diagonal = lax.broadcasted_iota(jnp.int32, (sub, sub), 0) == lax.broadcasted_iota(jnp.int32, (sub, sub), 1)
    lanes = lax.broadcasted_iota(jnp.int32, (sub, HD), 1)

    @pl.loop(0, n_mp)
    def _(mp):
        @pl.loop(0, n_dp)
        def _(dp):
            row = table[dp * n_mp + mp, pl.ds(my_dp, 1), :].astype(jnp.float32)
            column = jnp.sum(jnp.where(diagonal, row, 0.0), axis=1, keepdims=True).astype(jnp.int32)
            offset[mp, pl.ds(pl.multiple_of(dp * sub, sub), sub), :] = column - my_dp * group_rows - lanes

    acc[...] = jnp.zeros_like(acc)
    checks[last_slot : last_slot + PAIR] = jnp.zeros((PAIR,) + checks.shape[1:], jnp.float32)
    pieces = max(1, HD // sub)
    span = pieces * sub

    def arrival(step, mp):
        whole = landing.at[0, 0]
        return pltpu.make_async_copy(whole, whole, recv_sem.at[step, mp])

    def own_arrival(step):
        if n_dp > 1:
            part = landing.at[0, 0, pl.ds(0, n_dp - 1)]
            pltpu.make_async_copy(part, part, recv_sem.at[step, my_mp]).wait()

    @pl.loop(0, chunks)
    def _(step):
        first_slot = lax.rem(step * PAIR + per_device, slots)
        slot = step // last

        @pl.when(step + ahead < chunks)
        def _():
            issue(step + ahead)

        @pl.when(step < last)
        def _():
            own_arrival(step)

            @pl.loop(1, n_mp)
            def _(i):
                arrival(step, group_mp(i)).wait()

            fetch = pltpu.make_async_copy(landing.at[step], bufs.at[0], fetch_sem)
            fetch.start()
            fetch.wait()

        @pl.when(step == last)
        def _():
            sums[my_dp] = jnp.sum(checks[...], axis=1)

            @pl.loop(1, n_dp)
            def _(k):
                pltpu.make_async_remote_copy(
                    src_ref=sums.at[my_dp],
                    dst_ref=sums.at[my_dp],
                    send_sem=sum_send,
                    recv_sem=sum_recv,
                    device_id=(lax.rem(my_dp + k, n_dp), my_mp),
                    device_id_type=MESH,
                ).start()

            own_arrival(last)

        bufs[slot, my_mp, my_dp] = narrow[step, my_mp, my_dp]

        @pl.loop(0, n_mp)
        def _(i):
            mp = group_mp(i)

            @pl.when(slot * i > 0)
            def _():
                arrival(last, mp).wait()

            for b in range(n_dp // pieces):
                rows = bufs[slot, mp, pl.ds(b * pieces, pieces)].astype(jnp.float32).reshape(span, width)
                turned[:, pl.ds(b * span, span)] = rows.T.astype(jnp.bfloat16)

            @pl.loop(0, SLABS // UNROLL)
            def _(j):
                for u in range(UNROLL):
                    first = pl.multiple_of((j * UNROLL + u) * slab_rows, slab_rows)
                    marks = [
                        jnp.where(offset[mp] == first + t * HD, 1.0, 0.0).astype(jnp.bfloat16)
                        for t in range(slab_rows // HD)
                    ]
                    onehot = jnp.concatenate(marks, axis=1)
                    cols = pl.ds(first, slab_rows)
                    acc[:, cols] += jnp.dot(turned[...], onehot, preferred_element_type=jnp.float32)

        @pl.loop(0, SLABS)
        def _(s):
            rows = pl.ds(pl.multiple_of(s * slab_rows, slab_rows), slab_rows)
            block = acc[:, rows].astype(jnp.bfloat16)
            acc[:, rows] = jnp.zeros((width, slab_rows), jnp.float32)
            shards[pl.ds(first_slot, PAIR), :, rows] = block.reshape(PAIR, HD, slab_rows)
            projected = jnp.dot(block, probe[rows, :], preferred_element_type=jnp.float32)
            weighted = projected.reshape(PAIR, HD, -1) * lane[...].astype(jnp.float32)[None]
            slab_sums[s] = jnp.sum(weighted, axis=1)

        for s in range(SLABS):
            for pos in range(PAIR):
                checks[first_slot + pos, s : s + 1, :] = slab_sums[s, pos : pos + 1, :]

    tail_sums[my_dp, :PAIR] = jnp.sum(checks[last_slot : last_slot + PAIR], axis=1)

    @pl.loop(1, n_dp)
    def _(k):
        pltpu.make_async_remote_copy(
            src_ref=tail_sums.at[my_dp],
            dst_ref=tail_sums.at[my_dp],
            send_sem=tail_send,
            recv_sem=tail_recv,
            device_id=(lax.rem(my_dp + k, n_dp), my_mp),
            device_id_type=MESH,
        ).start()

    @pl.loop(0, chunks)
    def _(step):
        @pl.when(step >= 0)
        def _():
            part = narrow.at[0, 0]
            for m in range(n_mp - 1):
                pltpu.make_async_copy(part, part, send_sem.at[step]).wait()
            if n_dp > 1:
                part = narrow.at[0, 0, pl.ds(0, n_dp - 1)]
                pltpu.make_async_copy(part, part, send_sem.at[step]).wait()

    for buf, send, recv in ((sums, sum_send, sum_recv), (tail_sums, tail_send, tail_recv)):
        others = buf.at[pl.ds(0, n_dp - 1)]
        pltpu.make_async_copy(others, others, recv).wait()
        pltpu.make_async_copy(others, others, send).wait()
    total = sums[0]
    tail = tail_sums[0]
    for d in range(1, n_dp):
        total = total + sums[d]
        tail = tail + tail_sums[d]
    heads[...] = total / (n_dp * SLABS)
    heads[last_slot : last_slot + PAIR] = tail[:PAIR] / (n_dp * SLABS)


def write_out(shards, checks, heads, shards_out, checks_out, heads_out, sems):
    copies = [
        pltpu.make_async_copy(shards.at[h], shards_out.at[h], sems.at[h]) for h in range(shards.shape[0])
    ]
    copies.append(pltpu.make_async_copy(checks, checks_out, sems.at[shards.shape[0]]))
    copies.append(pltpu.make_async_copy(heads, heads_out, sems.at[shards.shape[0] + 1]))
    for copy in copies:
        copy.start()
    for copy in copies:
        copy.wait()


def body(stored, row_map, probe, lane):
    n_dp = lax.axis_size("dp")
    n_mp = lax.axis_size("mp")
    n_dev = n_dp * n_mp
    rows_dev = stored.shape[0]
    sub = rows_dev // n_dp
    group_rows, probes = probe.shape
    slots = Q_HEADS // n_mp + 2
    chunks = slots // PAIR
    width = PAIR * HD
    vmem = pl.BlockSpec(memory_space=pltpu.VMEM)
    hbm = pl.BlockSpec(memory_space=pl.ANY)
    shapes = (
        ((slots, HD, group_rows), jnp.bfloat16),
        ((slots, SLABS, probes), jnp.float32),
        ((slots, probes), jnp.float32),
    )
    kept = pl.pallas_call(
        functools.partial(exchange, n_dp, n_mp),
        out_shape=tuple(pltpu.VMEM(*s) for s in shapes)
        + (jax.ShapeDtypeStruct((chunks, n_mp, n_dp, sub, width), jnp.bfloat16),),
        in_specs=[hbm, hbm, hbm, hbm],
        out_specs=(vmem, vmem, vmem, hbm),
        scratch_shapes=[
            pltpu.VMEM((chunks, n_mp, n_dp, sub, width), jnp.bfloat16),
            pltpu.VMEM((n_mp, rows_dev, width), jnp.float32),
            pltpu.VMEM((2, n_mp, n_dp, sub, width), jnp.bfloat16),
            pltpu.VMEM((width, n_dp * sub), jnp.bfloat16),
            pltpu.VMEM((width, group_rows), jnp.float32),
            pltpu.VMEM((group_rows, probes), jnp.bfloat16),
            pltpu.VMEM(lane.shape, jnp.bfloat16),
            pltpu.VMEM((n_dev, n_dp, sub), jnp.int32),
            pltpu.VMEM((n_mp, n_dp * sub, HD), jnp.int32),
            pltpu.VMEM((SLABS, PAIR, probes), jnp.float32),
            pltpu.VMEM((n_dp, slots, probes), jnp.float32),
            pltpu.VMEM((n_dp, 8, probes), jnp.float32),
            pltpu.SemaphoreType.DMA((n_mp,)),
            pltpu.SemaphoreType.DMA((3,)),
            pltpu.SemaphoreType.DMA,
            pltpu.SemaphoreType.DMA((chunks,)),
            pltpu.SemaphoreType.DMA((chunks, n_mp)),
            pltpu.SemaphoreType.DMA,
            pltpu.SemaphoreType.DMA,
            pltpu.SemaphoreType.DMA,
            pltpu.SemaphoreType.DMA,
        ],
        compiler_params=pltpu.CompilerParams(
            collective_id=0, has_side_effects=True, vmem_limit_bytes=47_000_000
        ),
    )(stored, row_map.reshape(n_dev, n_dp, sub), probe, lane)
    return pl.pallas_call(
        write_out,
        out_shape=tuple(jax.ShapeDtypeStruct(*s) for s in shapes),
        in_specs=[vmem, vmem, vmem],
        out_specs=(hbm, hbm, hbm),
        scratch_shapes=[pltpu.SemaphoreType.DMA((slots + 2,))],
        compiler_params=pltpu.CompilerParams(vmem_limit_bytes=1_000_000),
    )(*kept[:3])


def solution(mesh):
    return jax.shard_map(
        body,
        mesh=mesh,
        in_specs=(P(("dp", "mp"), None), P(), P("dp", None), P()),
        out_specs=(P("mp", None, "dp"), P("mp", "dp", None), P("mp", None)),
        check_vma=False,
    )
```

```python
import functools

import jax
import jax.numpy as jnp
from jax import lax
from jax.experimental import pallas as pl
from jax.experimental.pallas import tpu as pltpu
from jax.sharding import PartitionSpec as P

Q_HEADS = 128
KV_HEADS = 8
HD = 128
SLABS = 8
PAIR = 2
AHEAD = 3
UNROLL = 4
FINAL = 2
PROBE_COLS = 256
MESH = pl.DeviceIdType.MESH


def exchange(
    n_dp, n_mp, stored, row_map, probe_any, lane_any,
    shards, checks, heads, landing,
    narrow, wide, bufs, turned, probe, lane, table, offset, late_turned, late_offset, late_onehot,
    slab_sums, sums, tail_sums,
    load_sem, aux_sem, fetch_sem, send_sem, recv_sem, late_sem, sum_send, sum_recv, tail_send, tail_recv,
):
    my_dp = lax.axis_index("dp")
    my_mp = lax.axis_index("mp")
    n_dev = n_dp * n_mp
    rows_dev = stored.shape[0]
    sub = rows_dev // n_dp
    group_rows = probe.shape[0]
    slab_rows = group_rows // SLABS
    per_device = Q_HEADS // n_mp
    slots = per_device + 2
    share = n_mp // KV_HEADS
    chunks = slots // PAIR
    last = chunks - 1
    width = PAIR * HD
    half = n_mp // 2
    my_half = my_mp // half
    part_rows = n_dp * sub
    ahead = min(AHEAD, chunks)
    last_slot = (last * PAIR + per_device) % slots
    near = half // 2
    pieces = max(1, HD // sub)
    span = pieces * sub
    late_each = max(1, HD // (near * sub))
    late_groups = n_dp // late_each

    quarter = my_mp // near
    middle = quarter * (3 - quarter) // 2

    def peer_mp(i):
        other = i // half
        side = (1 - my_half) * (1 - other) + my_half * other
        return side * half + lax.rem(my_mp + i, half)

    def group_mp(i):
        far = i // half
        inner = lax.rem(i, half)
        own = my_half * half + lax.rem(my_mp + inner, half)
        other = my_half * inner + (1 - my_half) * (n_mp - 1 - inner)
        return own * (1 - far) + other * far

    def load(step, i):
        mp = peer_mp(i)
        if isinstance(step, int) and step == 0:
            for pos, head in enumerate((Q_HEADS + mp // share, Q_HEADS + KV_HEADS + mp // share)):
                first = pl.multiple_of(head * HD, HD)
                src = stored.at[:, pl.ds(first, HD)]
                pltpu.make_async_copy(src, wide.at[i, :, pl.ds(pos * HD, HD)], load_sem.at[i]).start()
        else:
            first = pl.multiple_of((mp * per_device + (step - 1) * PAIR) * HD, HD)
            pltpu.make_async_copy(stored.at[:, pl.ds(first, width)], wide.at[i], load_sem.at[i]).start()

    def send(step, mp, dp, target, arrived):
        pltpu.make_async_remote_copy(
            src_ref=narrow.at[step, mp, dp],
            dst_ref=target,
            send_sem=send_sem.at[step],
            recv_sem=arrived,
            device_id=(dp, mp),
            device_id_type=MESH,
        ).start()

    def send_all(step, i):
        @pl.loop(0, n_dp)
        def _(a):
            @pl.when(i * n_dp + a != half * n_dp)
            def _():
                dp = lax.rem(my_dp + a, n_dp)
                send(step, peer_mp(i), dp, landing.at[step, my_mp, my_dp], recv_sem.at[step, my_mp])

    def send_last():
        @pl.loop(0, n_dp)
        def _(a):
            dp = lax.rem(my_dp + a, n_dp)

            @pl.loop(0, n_mp)
            def _(i):
                late = middle * (1 - i // half)

                @pl.when(late == 1)
                def _():
                    send(last, peer_mp(i), dp, bufs.at[1, my_mp, my_dp], late_sem.at[a // late_each])

                @pl.when(late == 0)
                def _():
                    @pl.when(i * n_dp + a != half * n_dp)
                    def _():
                        send(last, peer_mp(i), dp, bufs.at[1, my_mp, my_dp], recv_sem.at[last, my_mp])

    def issue(step):
        @pl.loop(0, n_mp)
        def _(i):
            mp = peer_mp(i)
            pltpu.make_async_copy(wide.at[i], wide.at[i], load_sem.at[i]).wait()

            @pl.loop(0, n_dp)
            def _(d):
                narrow[step, mp, d] = wide[i, pl.ds(pl.multiple_of(d * sub, sub), sub), :].astype(jnp.bfloat16)

            if not isinstance(step, int):
                @pl.when(step < last)
                def _():
                    send_all(step, i)
            elif step < last:
                send_all(step, i)

            if isinstance(step, int):
                if step < last:
                    load(step + 1, i)
            else:
                @pl.when(step < last)
                def _():
                    load(step + 1, i)

        if isinstance(step, int):
            if step == last:
                send_last()
        else:
            @pl.when(step == last)
            def _():
                send_last()

    @pl.loop(0, n_mp)
    def _(i):
        load(0, i)

    barrier = pltpu.get_barrier_semaphore()

    @pl.loop(1, n_dev)
    def _(k):
        other = (lax.rem(my_dp + k // n_mp, n_dp), lax.rem(my_mp + lax.rem(k, n_mp), n_mp))
        pl.semaphore_signal(barrier, inc=1, device_id=other, device_id_type=MESH)

    aux = (
        pltpu.make_async_copy(row_map, table, aux_sem.at[0]),
        pltpu.make_async_copy(lane_any, lane, aux_sem.at[1]),
        pltpu.make_async_copy(probe_any, probe, aux_sem.at[2]),
    )
    pl.semaphore_wait(barrier, n_dev - 1)
    issue(0)
    for copy in aux:
        copy.start()
    for step in range(1, ahead):
        issue(step)

    for copy in aux:
        copy.wait()
    diagonal = lax.broadcasted_iota(jnp.int32, (sub, sub), 0) == lax.broadcasted_iota(jnp.int32, (sub, sub), 1)
    lanes = lax.broadcasted_iota(jnp.int32, (sub, HD), 1)

    @pl.loop(0, n_mp)
    def _(mp):
        @pl.loop(0, n_dp)
        def _(dp):
            row = table[dp * n_mp + mp, pl.ds(my_dp, 1), :].astype(jnp.float32)
            column = jnp.sum(jnp.where(diagonal, row, 0.0), axis=1, keepdims=True).astype(jnp.int32)
            offset[mp, pl.ds(pl.multiple_of(dp * sub, sub), sub), :] = column - my_dp * group_rows - lanes

    def late_pieces(g):
        side = (1 - my_half) * half
        inner = my_half * near
        for k in range(late_each):
            dp = lax.rem(my_dp + n_dp - (g * late_each + k), n_dp)
            for m in range(near):
                yield side + inner + m, dp

    @pl.loop(0, late_groups)
    def _(g):
        for k, (mp, dp) in enumerate(late_pieces(g)):
            late_offset[g, k * sub : (k + 1) * sub, :] = offset[mp, pl.ds(pl.multiple_of(dp * sub, sub), sub), :]

    def onehot(numbers, first):
        marks = [
            jnp.where(numbers == first + t * HD, 1.0, 0.0).astype(jnp.bfloat16) for t in range(slab_rows // HD)
        ]
        return jnp.concatenate(marks, axis=1)

    @pl.loop(0, SLABS)
    def _(s):
        first = pl.multiple_of(s * slab_rows, slab_rows)
        late_onehot[:, pl.ds(first, slab_rows)] = onehot(late_offset[late_groups - 1], first)

    def turn(slot, mp):
        for b in range(n_dp // pieces):
            rows = bufs[slot, mp, pl.ds(b * pieces, pieces)].astype(jnp.float32).reshape(span, width)
            turned[:, pl.ds(b * span, span)] = rows.T.astype(jnp.bfloat16)

    def turn_late(g):
        rows = [bufs[1, mp, dp].astype(jnp.float32) for mp, dp in late_pieces(g)]
        late_turned[...] = jnp.concatenate(rows, axis=0).T.astype(jnp.bfloat16)

    def place(values, numbers, first_slot):
        @pl.loop(0, SLABS // UNROLL)
        def _(j):
            for u in range(UNROLL):
                first = pl.multiple_of((j * UNROLL + u) * slab_rows, slab_rows)
                cols = pl.ds(first, slab_rows)
                found = jnp.dot(values[...], onehot(numbers[...], first), preferred_element_type=jnp.float32)
                held = pl.ds(first_slot, PAIR)
                shards[held, :, cols] += found.astype(jnp.bfloat16).reshape(PAIR, HD, slab_rows)

    def finish(s, block):
        rows = pl.ds(pl.multiple_of(s * slab_rows, slab_rows), slab_rows)
        for p in range(0, probe.shape[1], PROBE_COLS):
            cols = slice(p, p + PROBE_COLS)
            projected = jnp.dot(block, probe[rows, cols], preferred_element_type=jnp.float32)
            weighted = projected.reshape(PAIR, HD, -1) * lane[:, cols].astype(jnp.float32)[None]
            slab_sums[s, :, cols] = jnp.sum(weighted, axis=1)

    def store_checks(first_slot):
        for s in range(SLABS):
            for pos in range(PAIR):
                checks[first_slot + pos, s : s + 1, :] = slab_sums[s, pos : pos + 1, :]

    @pl.loop(0, slots)
    def _(h):
        shards[h] = jnp.zeros(shards.shape[1:], jnp.bfloat16)

    def arrival(step, mp):
        whole = landing.at[0, 0]
        return pltpu.make_async_copy(whole, whole, recv_sem.at[step, mp])

    def own_arrival(step):
        if n_dp > 1:
            part = landing.at[0, 0, pl.ds(0, n_dp - 1)]
            pltpu.make_async_copy(part, part, recv_sem.at[step, my_mp]).wait()

    def slot_of(step):
        return lax.rem(step * PAIR + per_device, slots)

    def take(step, low, high):
        @pl.loop(low, high)
        def _(i):
            mp = group_mp(i)

            @pl.when(i > 0)
            def _():
                arrival(step, mp).wait()

            @pl.when(i == 0)
            def _():
                own_arrival(step)

        @pl.when(step < last)
        def _():
            @pl.loop(low, high)
            def _(i):
                mp = group_mp(i)
                pltpu.make_async_copy(landing.at[step, mp], bufs.at[0, mp], fetch_sem).start()

            part = landing.at[0, pl.ds(0, high - low)]
            pltpu.make_async_copy(part, part, fetch_sem).wait()

    def put(step, low, high):
        slot = step // last

        @pl.loop(low, high)
        def _(i):
            mp = group_mp(i)
            turn(slot, mp)
            place(turned, offset.at[mp], slot_of(step))

    def early(step):
        take(step, 0, n_mp - near)
        bufs[step // last, my_mp, my_dp] = narrow[step, my_mp, my_dp]
        put(step, 0, n_mp - near)

    early(0)

    @pl.loop(0, last)
    def _(step):
        @pl.when(step + ahead < chunks)
        def _():
            issue(step + ahead)

        early(step + 1)
        take(step, n_mp - near, n_mp)
        put(step, n_mp - near, n_mp)
        first_slot = slot_of(step)

        @pl.loop(0, SLABS // FINAL)
        def _(j):
            for u in range(FINAL):
                s = j * FINAL + u
                cols = pl.ds(pl.multiple_of(s * slab_rows, slab_rows), slab_rows)
                finish(s, shards[pl.ds(first_slot, PAIR), :, cols].reshape(width, slab_rows))

        store_checks(first_slot)

    checks[last_slot : last_slot + PAIR] = jnp.zeros((PAIR,) + checks.shape[1:], jnp.float32)
    sums[my_dp] = jnp.sum(checks[...], axis=1)

    @pl.loop(1, n_dp)
    def _(k):
        pltpu.make_async_remote_copy(
            src_ref=sums.at[my_dp],
            dst_ref=sums.at[my_dp],
            send_sem=sum_send,
            recv_sem=sum_recv,
            device_id=(lax.rem(my_dp + k, n_dp), my_mp),
            device_id_type=MESH,
        ).start()

    def late_arrival(g):
        part = landing.at[0, 0, pl.ds(0, late_each * near)]
        pltpu.make_async_copy(part, part, late_sem.at[g]).wait()

    @pl.loop(0, late_groups - 1)
    def _(g):
        late_arrival(g)
        turn_late(g)
        place(late_turned, late_offset.at[g], last_slot)

    late_arrival(late_groups - 1)
    turn_late(late_groups - 1)

    @pl.loop(0, SLABS // FINAL)
    def _(j):
        for u in range(FINAL):
            s = j * FINAL + u
            cols = pl.ds(pl.multiple_of(s * slab_rows, slab_rows), slab_rows)
            found = jnp.dot(late_turned[...], late_onehot[:, cols], preferred_element_type=jnp.float32)
            block = shards[last_slot : last_slot + PAIR, :, cols].reshape(width, slab_rows) + found.astype(jnp.bfloat16)
            shards[last_slot : last_slot + PAIR, :, cols] = block.reshape(PAIR, HD, slab_rows)
            finish(s, block)

    store_checks(last_slot)
    tail_sums[my_dp, :PAIR] = jnp.sum(checks[last_slot : last_slot + PAIR], axis=1)

    @pl.loop(1, n_dp)
    def _(k):
        pltpu.make_async_remote_copy(
            src_ref=tail_sums.at[my_dp],
            dst_ref=tail_sums.at[my_dp],
            send_sem=tail_send,
            recv_sem=tail_recv,
            device_id=(lax.rem(my_dp + k, n_dp), my_mp),
            device_id_type=MESH,
        ).start()

    @pl.loop(0, chunks)
    def _(step):
        @pl.when(step >= 0)
        def _():
            part = narrow.at[0, 0]
            for m in range(n_mp - 1):
                pltpu.make_async_copy(part, part, send_sem.at[step]).wait()
            if n_dp > 1:
                part = narrow.at[0, 0, pl.ds(0, n_dp - 1)]
                pltpu.make_async_copy(part, part, send_sem.at[step]).wait()

    for buf, send, recv in ((sums, sum_send, sum_recv), (tail_sums, tail_send, tail_recv)):
        others = buf.at[pl.ds(0, n_dp - 1)]
        pltpu.make_async_copy(others, others, recv).wait()
        pltpu.make_async_copy(others, others, send).wait()
    total = sums[0]
    tail = tail_sums[0]
    for d in range(1, n_dp):
        total = total + sums[d]
        tail = tail + tail_sums[d]
    heads[...] = total / (n_dp * SLABS)
    heads[last_slot : last_slot + PAIR] = tail[:PAIR] / (n_dp * SLABS)


def write_out(shards, checks, heads, shards_out, checks_out, heads_out, sems):
    copies = [
        pltpu.make_async_copy(shards.at[h], shards_out.at[h], sems.at[h]) for h in range(shards.shape[0])
    ]
    copies.append(pltpu.make_async_copy(checks, checks_out, sems.at[shards.shape[0]]))
    copies.append(pltpu.make_async_copy(heads, heads_out, sems.at[shards.shape[0] + 1]))
    for copy in copies:
        copy.start()
    for copy in copies:
        copy.wait()


def body(stored, row_map, probe, lane):
    n_dp = lax.axis_size("dp")
    n_mp = lax.axis_size("mp")
    n_dev = n_dp * n_mp
    rows_dev = stored.shape[0]
    sub = rows_dev // n_dp
    group_rows, probes = probe.shape
    slots = Q_HEADS // n_mp + 2
    chunks = slots // PAIR
    width = PAIR * HD
    near = n_mp // 4
    late_rows = near * sub * max(1, HD // (near * sub))
    vmem = pl.BlockSpec(memory_space=pltpu.VMEM)
    hbm = pl.BlockSpec(memory_space=pl.ANY)
    shapes = (
        ((slots, HD, group_rows), jnp.bfloat16),
        ((slots, SLABS, probes), jnp.float32),
        ((slots, probes), jnp.float32),
    )
    kept = pl.pallas_call(
        functools.partial(exchange, n_dp, n_mp),
        out_shape=tuple(pltpu.VMEM(*s) for s in shapes)
        + (jax.ShapeDtypeStruct((chunks, n_mp, n_dp, sub, width), jnp.bfloat16),),
        in_specs=[hbm, hbm, hbm, hbm],
        out_specs=(vmem, vmem, vmem, hbm),
        scratch_shapes=[
            pltpu.VMEM((chunks, n_mp, n_dp, sub, width), jnp.bfloat16),
            pltpu.VMEM((n_mp, rows_dev, width), jnp.float32),
            pltpu.VMEM((2, n_mp, n_dp, sub, width), jnp.bfloat16),
            pltpu.VMEM((width, n_dp * sub), jnp.bfloat16),
            pltpu.VMEM((group_rows, probes), jnp.bfloat16),
            pltpu.VMEM(lane.shape, jnp.bfloat16),
            pltpu.VMEM((n_dev, n_dp, sub), jnp.int32),
            pltpu.VMEM((n_mp, n_dp * sub, HD), jnp.int32),
            pltpu.VMEM((width, late_rows), jnp.bfloat16),
            pltpu.VMEM((n_dp * near * sub // late_rows, late_rows, HD), jnp.int32),
            pltpu.VMEM((late_rows, group_rows), jnp.bfloat16),
            pltpu.VMEM((SLABS, PAIR, probes), jnp.float32),
            pltpu.VMEM((n_dp, slots, probes), jnp.float32),
            pltpu.VMEM((n_dp, 8, probes), jnp.float32),
            pltpu.SemaphoreType.DMA((n_mp,)),
            pltpu.SemaphoreType.DMA((3,)),
            pltpu.SemaphoreType.DMA,
            pltpu.SemaphoreType.DMA((chunks,)),
            pltpu.SemaphoreType.DMA((chunks, n_mp)),
            pltpu.SemaphoreType.DMA((n_dp * near * sub // late_rows,)),
            pltpu.SemaphoreType.DMA,
            pltpu.SemaphoreType.DMA,
            pltpu.SemaphoreType.DMA,
            pltpu.SemaphoreType.DMA,
        ],
        compiler_params=pltpu.CompilerParams(
            collective_id=0, has_side_effects=True, vmem_limit_bytes=47_000_000
        ),
    )(stored, row_map.reshape(n_dev, n_dp, sub), probe, lane)
    return pl.pallas_call(
        write_out,
        out_shape=tuple(jax.ShapeDtypeStruct(*s) for s in shapes),
        in_specs=[vmem, vmem, vmem],
        out_specs=(hbm, hbm, hbm),
        scratch_shapes=[pltpu.SemaphoreType.DMA((slots + 2,))],
        compiler_params=pltpu.CompilerParams(vmem_limit_bytes=1_000_000),
    )(*kept[:3])


def solution(mesh):
    return jax.shard_map(
        body,
        mesh=mesh,
        in_specs=(P(("dp", "mp"), None), P(), P("dp", None), P()),
        out_specs=(P("mp", None, "dp"), P("mp", "dp", None), P("mp", None)),
        check_vma=False,
    )
```
